512 devices in a mesh: atoms: 128 (over z, x_lo, y), waves: 4 (over x_hi, core).
Axes of the slice: x: 4 (x_hi: 2, x_lo: 2; x = x_hi * 2 + x_lo), y: 8, z: 8, core: 2. Of those that a mesh axis runs over, the one named last changes fastest.
Arguments:
- features: bfloat16 [32768, 512], P('atoms'), may hold values from -6 to 6
- positions: int32 [3, 32768], P(None, 'atoms'), may hold values from 0 to 65535
- neighbours: int32 [256, 12], P('atoms'), may hold values from 0 to 255, as said below
- wavevectors: int32 [3, 4096], P(None, 'waves'), may hold values from -16 to 16
- radial_width: float32 [8], P('waves'), may hold values from 0.05 to 0.3
- short_weight: bfloat16 [8, 512, 512], P('waves'), may hold values from -0.09375 to 0.09375
- latent_weight: bfloat16 [512, 256], replicated, may hold values from -0.25 to 0.25
- mix_weight: float32 [256, 256], replicated, may hold values from -0.375 to 0.375
- filter_rate: float32 [256], replicated, may hold values from 0.0005 to 0.02
- out_weight: bfloat16 [256, 512], replicated, may hold values from -0.375 to 0.375
Outputs:
- message: bfloat16 [32768, 512], P('atoms', 'waves')
The draws below stay inside these ranges and needn't reach their ends.
Inputs may be any that keep to these rules, and one draw needn't show every extreme that they name: `neighbours`: row b holds 12 different block numbers, each within 7 blocks of b counted cyclically over the 256 blocks; b itself may appear.
All inputs are finite; a program needn't handle non-finite values.
Results may differ from the reference program's by a relative error of at most 0.012.
Values may be sent and summed in bfloat16 or wider, within the bound.
No kernel may reach another device: no remote copies, remote signals or barrier semaphores. Data moves between devices by JAX's collectives and lax.ppermute only.
A program may use at most 64 MiB of HBM per device.

```python
import math
import jax
import jax.numpy as jnp
from jax import lax

C = 512
LAT = 256
K = 4096
RADIAL = 8
BLOCK = 128
NBR = 12
REACH = 7
NBLOCKS = 256
NATOMS = 32768
N_WAVES = 4


def draw_neighbours(key, part):
    pop_key, pick_key = jax.random.split(jax.random.fold_in(key, 11))
    span = 2 * REACH + 1
    popularity = jax.random.randint(pop_key, (NBLOCKS,), 0, 4096)
    jitter = jax.random.randint(pick_key, (NBLOCKS, span), 0, 1024)
    shifts = jnp.arange(span, dtype=jnp.int32) - REACH
    block_ids = jnp.arange(NBLOCKS, dtype=jnp.int32)
    target = jnp.mod(block_ids[:, None] + shifts[None, :], NBLOCKS)
    scores = (jitter + popularity[target]) * 32 + (shifts[None, :] + REACH)
    _, picked = lax.top_k(-scores, NBR)
    return jnp.take_along_axis(target, picked, axis=1).astype(jnp.int32)


def with_ends(entries, stream_key, smallest, high):
    place = [jax.random.randint(jax.random.fold_in(stream_key, axis), (), 0, length) for axis, length in enumerate(entries.shape)]
    widest = entries.shape.index(max(entries.shape))
    beside = place[:widest] + [(place[widest] + 1) % entries.shape[widest]] + place[widest + 1:]
    return entries.at[tuple(place)].set(smallest).at[tuple(beside)].set(high)


def shard_levels(key, shape, shards, least, top_value):
    def one(position, shards_of):
        heights = jax.random.uniform(jax.random.fold_in(jax.random.fold_in(key, 6), position), (shards_of,), jnp.float32, least / len(shards), top_value / len(shards))
        return jnp.repeat(jnp.exp(heights), shape[position] // shards_of).reshape((-1,) + (1,) * (len(shape) - position - 1))

    level = one(*shards[0])
    for cut in shards[1:]:
        level = level * one(*cut)
    return level


def noise(stream_key, dims, deviation, reach, pieces=(), kind=jnp.bfloat16):
    values = jax.random.normal(stream_key, dims, jnp.float32) * deviation
    if len(pieces) > 0:
        values = shard_levels(stream_key, dims, pieces, -0.22, 0.18) * values
    return jnp.clip(values, min=-reach, max=reach).astype(kind)


def setup_inputs(seed: int = 0) -> dict:
    key_list = jax.random.split(jax.random.key(seed), 11)
    features = noise(key_list[0], (NATOMS, C), 1.0, 6.0, ((0, 128),))
    positions = with_ends(jax.random.randint(key_list[1], (3, NATOMS), 0, 65536), jax.random.fold_in(key_list[1], 1), 0, 65535).astype(jnp.int32)
    neighbours = draw_neighbours(jax.random.fold_in(key_list[10], 71), 0)
    wavevectors = with_ends(jax.random.randint(key_list[3], (3, K), -16, 17), jax.random.fold_in(key_list[3], 1), -16, 16).astype(jnp.int32)
    radial_width = jnp.clip(jnp.exp(math.log(0.3) - 1.7917595 * jax.random.uniform(key_list[4], (RADIAL,), jnp.float32) ** shard_levels(key_list[4], (RADIAL,), ((0, 4),), -0.2, 0.2)), 0.05, 0.3)
    short_weight = noise(key_list[5], (RADIAL, C, C), (RADIAL * C) ** -0.5, 0.09375, ((0, 4),))
    latent_weight = noise(key_list[6], (C, LAT), C ** -0.5, 0.25)
    mix_weight = noise(key_list[7], (LAT, LAT), LAT ** -0.5, 0.375, (), jnp.float32)
    filter_rate = jnp.clip(jnp.exp(jax.random.uniform(key_list[8], (LAT,), jnp.float32, math.log(0.0005), math.log(0.02))), 0.0005, 0.02)
    out_weight = noise(key_list[9], (LAT, C), LAT ** -0.5, 0.375)
    return dict(features=features, positions=positions, neighbours=neighbours, wavevectors=wavevectors, radial_width=radial_width, short_weight=short_weight, latent_weight=latent_weight, mix_weight=mix_weight, filter_rate=filter_rate, out_weight=out_weight)


cutoff = 0.5

def kernels(own_pos, near_pos, centers, radial_width):
    offsets = own_pos[:, None, :, None] - near_pos[:, :, None, :]
    offsets = jnp.mod(offsets, 65536)
    offsets = jnp.where(offsets >= 32768, offsets - 65536, offsets)
    coords = offsets.astype(jnp.float32) * (1.0 / 65536.0)
    dist_sq = lax.optimization_barrier(jnp.sum(coords * coords, axis=0))
    distance = jnp.sqrt(dist_sq)
    smooth = jnp.where(dist_sq < cutoff * cutoff, jnp.square(1.0 - dist_sq / (cutoff * cutoff)), 0.0)
    shaped = (distance[None] - centers[:, None, None, None]) / radial_width[:, None, None, None]
    norm_scale = 1.0 / math.sqrt(NBR * BLOCK)
    return (jnp.exp(-jnp.square(shaped)) * smooth[None] * norm_scale).astype(jnp.bfloat16)

def phases_of(wavevectors, spots):
    phase_turn = wavevectors[0][:, None] * spots[0][None, :] + wavevectors[1][:, None] * spots[1][None, :] + wavevectors[2][:, None] * spots[2][None, :]
    phase_turn = jnp.mod(phase_turn, 65536)
    angles = phase_turn.astype(jnp.float32) * (2.0 * math.pi / 65536.0)
    return jnp.concatenate([jnp.cos(angles), jnp.sin(angles)], axis=0).astype(jnp.bfloat16)

def filter_gain(wavevectors, filter_rate):
    lengths = lax.optimization_barrier(jnp.sum(wavevectors * wavevectors, axis=0)).astype(jnp.float32)
    return jnp.exp(-lengths[:, None] * filter_rate[None, :])

def reference(features, positions, neighbours, wavevectors, radial_width, short_weight, latent_weight, mix_weight, filter_rate, out_weight):
    block_count = neighbours.shape[0]
    feat_blocks = features.reshape(block_count, BLOCK, C)
    pos_blocks = positions.reshape(3, block_count, BLOCK)
    centers = cutoff * jnp.arange(RADIAL).astype(jnp.float32) / (RADIAL - 1)
    flat_weight = short_weight.reshape(RADIAL * C, C)

    def short_block(block_index):
        near_blocks = neighbours[block_index]
        near_feat = feat_blocks[near_blocks]
        near_pos = pos_blocks[:, near_blocks]
        weights = kernels(pos_blocks[:, block_index], near_pos, centers, radial_width)
        gathered = jnp.einsum('rjia,jac->irc', weights.astype(jnp.float32), near_feat.astype(jnp.float32))
        gathered = gathered.astype(jnp.bfloat16).reshape(BLOCK, RADIAL * C)
        return jnp.dot(gathered, flat_weight, preferred_element_type=jnp.float32)
    block_ids = jnp.arange(block_count, dtype=jnp.int32)
    short_range = lax.map(short_block, block_ids).reshape(block_count * BLOCK, C)
    latent = jnp.dot(features, latent_weight, preferred_element_type=jnp.float32).astype(jnp.bfloat16)
    lat_blocks = latent.reshape(block_count, BLOCK, LAT)

    def add_factor(running, block_index):
        phases = phases_of(wavevectors, pos_blocks[:, block_index])
        return (running + jnp.dot(phases, lat_blocks[block_index], preferred_element_type=jnp.float32), None)
    factors, _ = lax.scan(add_factor, jnp.zeros((2 * K, LAT), jnp.float32), block_ids)
    gain = filter_gain(wavevectors, filter_rate)
    gain = jnp.concatenate([gain, gain], axis=0)
    norm_scale = 1.0 / math.sqrt(block_count * BLOCK)
    mixed = jnp.dot(factors, mix_weight, precision=lax.Precision.HIGHEST)
    filtered = (gain * mixed * norm_scale).astype(jnp.bfloat16)
    group_size = K // N_WAVES

    def long_block(block_index):
        phases = phases_of(wavevectors, pos_blocks[:, block_index])
        running = jnp.zeros((BLOCK, C), jnp.float32)
        for wave_group in range(N_WAVES):
            low = wave_group * group_size
            group_rows = jnp.concatenate([phases[low:low + group_size], phases[K + low:K + low + group_size]], axis=0)
            group_filter = jnp.concatenate([filtered[low:low + group_size], filtered[K + low:K + low + group_size]], axis=0)
            summed = lax.dot_general(group_rows, group_filter, (((0,), (0,)), ((), ())), preferred_element_type=jnp.float32)
            summed = (summed * (1.0 / math.sqrt(K))).astype(jnp.bfloat16)
            running = running + jnp.dot(summed, out_weight, preferred_element_type=jnp.float32)
        return running
    long_range = lax.map(long_block, block_ids).reshape(block_count * BLOCK, C)
    return (short_range + long_range).astype(jnp.bfloat16)
```

```python
import math

import jax
import jax.numpy as jnp
from jax import lax
from jax.experimental import pallas as pl
from jax.experimental.pallas import tpu as pltpu
from jax.sharding import Mesh
from jax.sharding import PartitionSpec as P

K = 4096
RADIAL = 8
BLOCK = 128
NBR = 12
NATOMS = 32768
CUTOFF = 0.5
ATOMS = ("z", "xlo", "y")
WAVES = ("xhi", "core")
ROWS = 144

SIN_PI = (
    3.1415926535362884,
    -5.167712764624537,
    2.5501633189471584,
    -0.5992521978252471,
    0.08205040181554192,
    -0.00702838642033113,
)


def sin_pi(v):
    square = v * v
    total = jnp.float32(SIN_PI[-1])
    for coefficient in SIN_PI[-2::-1]:
        total = total * square + jnp.float32(coefficient)
    return total * v


def phases_of(waves, spots):
    turn = (
        waves[0][:, None] * spots[0][None, :]
        + waves[1][:, None] * spots[1][None, :]
        + waves[2][:, None] * spots[2][None, :]
    )
    share = turn * (1.0 / 65536.0)
    share = share - jnp.floor(share + 0.5)
    cosine = sin_pi(0.5 - 2.0 * jnp.abs(share))
    shifted = share - 0.25
    shifted = shifted - jnp.floor(shifted + 0.5)
    sine = sin_pi(0.5 - 2.0 * jnp.abs(shifted))
    return jnp.concatenate([cosine, sine], axis=0).astype(jnp.bfloat16)


def short_kernel(slots, coef, own, window, weight, out, spread, source):
    for block in range(2):
        rows = slice(block * BLOCK, (block + 1) * BLOCK)
        for j in range(NBR):
            slot = slots[block, j]
            near = window[slot, BLOCK : BLOCK + 16, :].astype(jnp.float32)
            dist_sq = None
            for axis in range(3):
                spot = near[axis : axis + 1] * 256.0 + near[axis + 3 : axis + 4]
                gap = own[rows, axis : axis + 1] - spot
                gap = gap - 65536.0 * jnp.floor(gap * (1.0 / 65536.0) + 0.5)
                gap = gap * (1.0 / 65536.0)
                dist_sq = gap * gap if dist_sq is None else dist_sq + gap * gap
            distance = jnp.sqrt(dist_sq)
            fade = 1.0 - dist_sq * 4.0
            smooth = jnp.where(
                dist_sq < CUTOFF * CUTOFF, fade * fade * (1.0 / math.sqrt(NBR * BLOCK)), 0.0
            )
            for r in range(RADIAL):
                shaped = (distance - CUTOFF * r / (RADIAL - 1)) * coef[0, r]
                value = jnp.exp(-(shaped * shaped)) * smooth
                spread[r * BLOCK : (r + 1) * BLOCK, j * BLOCK : (j + 1) * BLOCK] = value.astype(
                    jnp.bfloat16
                )
            source[j * BLOCK : (j + 1) * BLOCK, :] = window[slot, 0:BLOCK, :]
        gathered = jnp.dot(spread[...], source[...], preferred_element_type=jnp.float32)
        gathered = gathered.astype(jnp.bfloat16)
        gathered = jnp.concatenate(
            [gathered[r * BLOCK : (r + 1) * BLOCK] for r in range(RADIAL)], axis=1
        )
        out[rows, :] = jnp.dot(gathered, weight[...], preferred_element_type=jnp.float32)


def short_range_of(slots, coef, own, window, weight):
    return pl.pallas_call(
        short_kernel,
        out_shape=jax.ShapeDtypeStruct((2 * BLOCK, weight.shape[1]), jnp.float32),
        in_specs=[
            pl.BlockSpec(memory_space=pltpu.SMEM),
            pl.BlockSpec(memory_space=pltpu.SMEM),
            pl.BlockSpec(memory_space=pltpu.VMEM),
            pl.BlockSpec(memory_space=pltpu.VMEM),
            pl.BlockSpec(memory_space=pltpu.VMEM),
        ],
        out_specs=pl.BlockSpec(memory_space=pltpu.VMEM),
        scratch_shapes=[
            pltpu.VMEM((RADIAL * BLOCK, NBR * BLOCK), jnp.bfloat16),
            pltpu.VMEM((NBR * BLOCK, BLOCK), jnp.bfloat16),
        ],
        cost_estimate=pl.CostEstimate(
            flops=1100000000, bytes_accessed=3000000, transcendentals=3500000
        ),
        name="short_range",
    )(slots, coef, own, window, weight)


def exchanged(pieces, axes):
    return lax.all_to_all(pieces, axes, split_axis=0, concat_axis=0, tiled=True)


def coded(spots):
    digits = jnp.concatenate([spots >> 8, spots & 255], axis=0)
    return digits.astype(jnp.bfloat16)


def local(
    features,
    positions,
    neighbours,
    wavevectors,
    radial_width,
    short_weight,
    latent_weight,
    mix_weight,
    filter_rate,
    out_weight,
):
    xlo = lax.axis_index("xlo")
    y = lax.axis_index("y")
    wave = lax.axis_index(WAVES)
    atoms, channels = features.shape
    latents = latent_weight.shape[1]
    rows_count = lax.axis_size("z") * lax.axis_size("xlo")
    columns = lax.axis_size("y")
    wave_devices = lax.axis_size(WAVES)
    part = channels // wave_devices

    latent = jnp.dot(features, latent_weight, preferred_element_type=jnp.float32).astype(
        jnp.bfloat16
    )
    digits = coded(positions)
    packet = jnp.concatenate(
        [latent, digits, jnp.zeros((10, latents), jnp.bfloat16)], axis=0
    )
    arrived = lax.ppermute(packet, "xlo", [(0, 1), (1, 0)])
    other_latent = arrived[:atoms]
    other_digits = arrived[atoms : atoms + 6].astype(jnp.float32)
    other_spots = other_digits[0:3] * 256.0 + other_digits[3:6]

    own_part = lax.dynamic_slice_in_dim(features, wave * part, part, axis=1)
    block_digits = jnp.moveaxis(digits.reshape(6, 2, BLOCK), 1, 0)
    block_digits = jnp.pad(block_digits, ((0, 0), (0, ROWS - BLOCK - 6), (0, 0)))
    mine = jnp.concatenate([own_part.reshape(2, BLOCK, part), block_digits], axis=1)
    pairs = [
        (
            row * columns + column,
            (row + (-1 if column < columns // 2 else 1)) % rows_count * columns + column,
        )
        for row in range(rows_count)
        for column in range(columns)
    ]
    beside = lax.ppermute(mine, ATOMS, pairs)

    ahead = y - jnp.arange(columns, dtype=jnp.int32)
    use_mine = jnp.stack(
        [(ahead > -4) & (ahead <= 4), (ahead >= -4) & (ahead < 4)], axis=1
    )
    window = jnp.where(use_mine[:, :, None, None], mine[None], beside[None])
    window = exchanged(window, "y").reshape(2 * columns, ROWS, part)

    high = lax.reduce_precision(radial_width, 8, 7)
    middle = lax.reduce_precision(radial_width - high, 8, 7)
    low = radial_width - high - middle
    widths = jnp.stack([high, middle, low]).reshape(1, 6).astype(jnp.bfloat16)
    widths = jnp.pad(widths, ((0, 15), (0, channels - 6)))
    maps = jnp.moveaxis(short_weight.reshape(2, wave_devices, part, channels), 1, 0)
    maps = maps.reshape(wave_devices, 2 * part, channels)
    maps = jnp.concatenate(
        [maps, jnp.broadcast_to(widths, (wave_devices, 16, channels))], axis=1
    )
    maps = exchanged(maps, WAVES)
    width_digits = maps[:, 2 * part, :6].astype(jnp.float32).reshape(wave_devices, 3, 2)
    width = (width_digits[:, 0] + width_digits[:, 1] + width_digits[:, 2]).reshape(1, RADIAL)
    flat_weight = maps[:, : 2 * part].reshape(RADIAL * part, channels)

    spots = positions.astype(jnp.float32)
    own_columns = jnp.pad(spots.T, ((0, 0), (0, 5)))
    short_range = short_range_of(
        neighbours & (2 * columns - 1), 1.0 / width, own_columns, window, flat_weight
    )

    half = wavevectors.shape[1] // 2
    waves = lax.dynamic_slice_in_dim(wavevectors, xlo * half, half, axis=1)
    float_waves = waves.astype(jnp.float32)
    own_phases = phases_of(float_waves, spots)
    other_phases = phases_of(float_waves, other_spots)
    partial = jnp.dot(own_phases, latent, preferred_element_type=jnp.float32) + jnp.dot(
        other_phases, other_latent, preferred_element_type=jnp.float32
    )
    owners = ("z", "y")
    count = lax.axis_size(owners)
    lines = 2 * half // count
    pieces = exchanged(partial.astype(jnp.bfloat16).reshape(count, lines, latents), owners)
    factors = jnp.sum(pieces.astype(jnp.float32), axis=0)
    mixed = jnp.dot(factors, mix_weight, precision=lax.Precision.HIGHEST)
    first = lax.rem(lax.axis_index(owners) * lines, half)
    filter_waves = lax.dynamic_slice_in_dim(waves, first, lines, axis=1)
    lengths = jnp.sum(filter_waves * filter_waves, axis=0).astype(jnp.float32)
    gain = jnp.exp(-lengths[:, None] * filter_rate[None, :])
    filtered = (gain * mixed * (1.0 / math.sqrt(NATOMS))).astype(jnp.bfloat16)
    filtered = exchanged(jnp.broadcast_to(filtered, (count, lines, latents)), owners)
    filtered = filtered.reshape(2 * half, latents)

    def back(phases):
        summed = lax.dot_general(
            phases, filtered, (((0,), (0,)), ((), ())), preferred_element_type=jnp.float32
        )
        summed = (summed * (1.0 / math.sqrt(K))).astype(jnp.bfloat16)
        return jnp.dot(summed, out_weight, preferred_element_type=jnp.float32)

    own_message = (back(own_phases) + short_range).astype(jnp.bfloat16)
    other_message = back(other_phases).astype(jnp.bfloat16)
    first_is_mine = xlo == 0
    message = jnp.stack(
        [
            jnp.where(first_is_mine, own_message, other_message),
            jnp.where(first_is_mine, other_message, own_message),
        ]
    )
    message = jnp.moveaxis(message.reshape(2, atoms, wave_devices, part), 2, 1)
    message = exchanged(message.reshape(2 * wave_devices, atoms, part), ("xlo", *WAVES))
    return jnp.sum(message.astype(jnp.float32), axis=0).astype(jnp.bfloat16)


def solution(mesh):
    torus = Mesh(mesh.devices.reshape(8, 2, 8, 2, 2), (*ATOMS, *WAVES))
    placed = (
        P(ATOMS, None),
        P(None, ATOMS),
        P(ATOMS, None),
        P(None, WAVES),
        P(WAVES),
        P(WAVES, None, None),
        P(),
        P(),
        P(),
        P(),
    )
    return jax.shard_map(
        local, mesh=torus, in_specs=placed, out_specs=P(ATOMS, WAVES), check_vma=False
    )
```

```python
import math

import jax
import jax.numpy as jnp
from jax import lax
from jax.experimental import pallas as pl
from jax.experimental.pallas import tpu as pltpu
from jax.sharding import Mesh
from jax.sharding import PartitionSpec as P


K = 4096
RADIAL = 8
BLOCK = 128
NBR = 12
NATOMS = 32768
CUTOFF = 0.5
ATOMS = ("z", "xlo", "y")
WAVES = ("xhi", "core")
ROWS = 144

SIN_PI = (
    3.1415926535362884,
    -5.167712764624537,
    2.5501633189471584,
    -0.5992521978252471,
    0.08205040181554192,
    -0.00702838642033113,
)


def sin_pi(v):
    square = v * v
    total = jnp.float32(SIN_PI[-1])
    for coefficient in SIN_PI[-2::-1]:
        total = total * square + jnp.float32(coefficient)
    return total * v


def phases_of(waves, spots):
    turn = (
        waves[0][:, None] * spots[0][None, :]
        + waves[1][:, None] * spots[1][None, :]
        + waves[2][:, None] * spots[2][None, :]
    )
    share = turn * (1.0 / 65536.0)
    share = share - jnp.floor(share + 0.5)
    cosine = sin_pi(0.5 - 2.0 * jnp.abs(share))
    shifted = share - 0.25
    shifted = shifted - jnp.floor(shifted + 0.5)
    sine = sin_pi(0.5 - 2.0 * jnp.abs(shifted))
    return jnp.concatenate([cosine, sine], axis=0).astype(jnp.bfloat16)


WINDOW_ROWS = 2 * ROWS
MAP_ROWS = 8 * BLOCK + 16


def map_rows(ref, first):
    quarters = [ref[first + q * 256 : first + (q + 1) * 256, :] for q in range(4)]
    return jnp.concatenate(quarters, axis=1)


def prepare_kernel(
    table, width, features, positions, weights, latent_weight, packet, mine, left, right, maps0, maps2
):
    wave = table[0]
    latent = jnp.dot(features[...], latent_weight[...], preferred_element_type=jnp.float32)
    spots = positions[...]
    digits = jnp.concatenate(
        [spots >> 8, spots & 255, jnp.zeros((10, spots.shape[1]), jnp.int32)], axis=0
    )
    digits = digits.astype(jnp.float32).astype(jnp.bfloat16)
    atoms = latent.shape[0]
    packet[0:atoms, :] = latent.astype(jnp.bfloat16)
    packet[atoms : atoms + 16, :] = digits

    row = lax.broadcasted_iota(jnp.int32, (16, BLOCK), 0)
    sharp = jnp.where(row % 2 == 0, width[0], width[1])
    sharp = 1.0 / sharp
    high = sharp.astype(jnp.bfloat16).astype(jnp.float32)
    middle = (sharp - high).astype(jnp.bfloat16).astype(jnp.float32)
    low = sharp - high - middle
    sharp = jnp.where(row < 2, high, jnp.where(row < 4, middle, jnp.where(row < 6, low, 0.0)))
    sharp = sharp.astype(jnp.bfloat16)

    def put_maps(out, first, target):
        start = pl.multiple_of(target * BLOCK, BLOCK)
        for i in range(2):
            for q in range(4):
                at = first + q * 256 + i * BLOCK
                out[at : at + BLOCK, :] = weights[
                    i, pl.ds(start, BLOCK), q * BLOCK : (q + 1) * BLOCK
                ]
        out[first + 1024 : first + 1040, :] = sharp

    def put_window(out, target):
        start = pl.multiple_of(target * BLOCK, BLOCK)
        for block in range(2):
            rows = slice(block * BLOCK, (block + 1) * BLOCK)
            out[block * ROWS : block * ROWS + BLOCK, :] = features[rows, pl.ds(start, BLOCK)]
            out[block * ROWS + BLOCK : (block + 1) * ROWS, :] = digits[:, rows]

    put_window(mine, wave)
    put_window(left, wave ^ 1)
    put_maps(left, WINDOW_ROWS, wave ^ 1)
    put_window(right, wave ^ 3)
    put_maps(right, WINDOW_ROWS, wave ^ 3)
    put_maps(maps0, 0, wave)
    put_maps(maps2, 0, wave ^ 2)


def prepared(wave, radial_width, features, positions, short_weight, latent_weight):
    in_vmem = pl.BlockSpec(memory_space=pltpu.VMEM)
    in_smem = pl.BlockSpec(memory_space=pltpu.SMEM)
    atoms = features.shape[0]
    shapes = [
        (atoms + 16, latent_weight.shape[1]),
        (WINDOW_ROWS, BLOCK),
        (WINDOW_ROWS + MAP_ROWS, BLOCK),
        (WINDOW_ROWS + MAP_ROWS, BLOCK),
        (MAP_ROWS, BLOCK),
        (MAP_ROWS, BLOCK),
    ]
    return pl.pallas_call(
        prepare_kernel,
        out_shape=[jax.ShapeDtypeStruct(shape, jnp.bfloat16) for shape in shapes],
        in_specs=[in_smem, in_smem, in_vmem, in_vmem, in_vmem, in_vmem],
        out_specs=[in_vmem] * 6,
        cost_estimate=pl.CostEstimate(flops=67000000, bytes_accessed=3500000, transcendentals=0),
        name="prepare",
    )(wave, radial_width, features, positions, short_weight, latent_weight)


def short_kernel(table, before, left, mine, right, after, maps0, maps2, out, window, spread, source):
    window[0 : 5 * ROWS] = before[...]
    window[5 * ROWS : 7 * ROWS] = left[0:WINDOW_ROWS]
    window[7 * ROWS : 9 * ROWS] = mine[...]
    window[9 * ROWS : 11 * ROWS] = right[0:WINDOW_ROWS]
    window[11 * ROWS : 16 * ROWS] = after[...]
    maps = ((maps0, 0), (left, WINDOW_ROWS), (maps2, 0), (right, WINDOW_ROWS))
    wave = table[0, NBR]
    centers = []
    sharpness = []
    for p in range(4):
        ref, first = maps[p]
        digits = ref[first + 1024 : first + 1040, :].astype(jnp.float32)
        for i in range(2):
            kernel_id = (2 * (wave ^ p) + i).astype(jnp.float32)
            centers.append(kernel_id * (CUTOFF / (RADIAL - 1)))
            sharpness.append(digits[i : i + 1] + digits[i + 2 : i + 3] + digits[i + 4 : i + 5])
    for block in range(2):
        rows = slice(block * BLOCK, (block + 1) * BLOCK)
        digits = mine[block * ROWS + BLOCK : (block + 1) * ROWS, :].astype(jnp.float32)
        spots = digits[0:3] * 256.0 + digits[3:6]
        spots = jnp.concatenate([spots, jnp.zeros((BLOCK - 3, BLOCK), jnp.float32)], axis=0).T
        for j in range(NBR):
            start = pl.multiple_of(table[block, j] * ROWS, 16)
            near = window[pl.ds(start + BLOCK, 16), :].astype(jnp.float32)
            dist_sq = None
            for axis in range(3):
                spot = near[axis : axis + 1] * 256.0 + near[axis + 3 : axis + 4]
                gap = spots[:, axis : axis + 1] - spot
                gap = gap - 65536.0 * jnp.floor(gap * (1.0 / 65536.0) + 0.5)
                gap = gap * (1.0 / 65536.0)
                dist_sq = gap * gap if dist_sq is None else dist_sq + gap * gap
            distance = jnp.sqrt(dist_sq)
            fade = 1.0 - dist_sq * 4.0
            smooth = jnp.where(
                dist_sq < CUTOFF * CUTOFF, fade * fade * (1.0 / math.sqrt(NBR * BLOCK)), 0.0
            )
            for r in range(RADIAL):
                shaped = (distance - centers[r]) * sharpness[r]
                value = jnp.exp(-(shaped * shaped)) * smooth
                spread[r * BLOCK : (r + 1) * BLOCK, j * BLOCK : (j + 1) * BLOCK] = value.astype(
                    jnp.bfloat16
                )
            source[j * BLOCK : (j + 1) * BLOCK, :] = window[pl.ds(start, BLOCK), :]
        gathered = jnp.dot(spread[...], source[...], preferred_element_type=jnp.float32)
        gathered = gathered.astype(jnp.bfloat16)
        total = None
        for p in range(4):
            pair = jnp.concatenate(
                [
                    gathered[2 * p * BLOCK : (2 * p + 1) * BLOCK],
                    gathered[(2 * p + 1) * BLOCK : (2 * p + 2) * BLOCK],
                ],
                axis=1,
            )
            share = jnp.dot(pair, map_rows(*maps[p]), preferred_element_type=jnp.float32)
            total = share if total is None else total + share
        out[rows, :] = total


def short_range_of(table, before, left, mine, right, after, maps0, maps2):
    in_vmem = pl.BlockSpec(memory_space=pltpu.VMEM)
    return pl.pallas_call(
        short_kernel,
        out_shape=jax.ShapeDtypeStruct((2 * BLOCK, 4 * BLOCK), jnp.float32),
        in_specs=[pl.BlockSpec(memory_space=pltpu.SMEM)] + [in_vmem] * 7,
        out_specs=in_vmem,
        scratch_shapes=[
            pltpu.VMEM((16 * ROWS, BLOCK), jnp.bfloat16),
            pltpu.VMEM((RADIAL * BLOCK, NBR * BLOCK), jnp.bfloat16),
            pltpu.VMEM((NBR * BLOCK, BLOCK), jnp.bfloat16),
        ],
        cost_estimate=pl.CostEstimate(
            flops=1100000000, bytes_accessed=3000000, transcendentals=3500000
        ),
        name="short_range",
    )(table, before, left, mine, right, after, maps0, maps2)


def exchanged(pieces, axes):
    return lax.all_to_all(pieces, axes, split_axis=0, concat_axis=0, tiled=True)


def moved(value, steps, wave_flip=0, atom_flip=0):
    count = lax.axis_size(ATOMS)
    waves = lax.axis_size(WAVES)
    pairs = [
        (
            device * waves + wave,
            (((device ^ atom_flip) + steps) % count) * waves + (wave ^ wave_flip),
        )
        for device in range(count)
        for wave in range(waves)
    ]
    return lax.ppermute(value, ATOMS + WAVES, pairs)


def local(
    features,
    positions,
    neighbours,
    wavevectors,
    radial_width,
    short_weight,
    latent_weight,
    mix_weight,
    filter_rate,
    out_weight,
):
    xlo = lax.axis_index("xlo")
    device = lax.axis_index(ATOMS)
    wave = lax.axis_index(WAVES).astype(jnp.int32)
    atoms, channels = features.shape
    latents = latent_weight.shape[1]
    wave_devices = lax.axis_size(WAVES)
    part = channels // wave_devices
    partner = lax.axis_size("y")

    packet, mine, to_right, to_left, maps0, maps2 = prepared(
        wave.reshape(1), radial_width, features, positions, short_weight, latent_weight
    )
    latent = packet[:atoms]
    arrived = moved(packet, 0, 0, partner)
    other_latent = arrived[:atoms]
    other_digits = arrived[atoms : atoms + 6].astype(jnp.float32)
    other_spots = other_digits[0:3] * 256.0 + other_digits[3:6]

    left = moved(to_right, 1, 1)
    right = moved(to_left, -1, 3)
    maps2 = moved(maps2, 0, 2, partner)
    sent_on = jnp.concatenate([left[ROWS:WINDOW_ROWS], mine, right[:WINDOW_ROWS]])
    sent_back = jnp.concatenate([left[:WINDOW_ROWS], mine, right[:ROWS]])
    before = moved(sent_on, 3)
    after = moved(sent_back, -3)

    slots = (neighbours - (2 * device - 7)) & 15
    table = jnp.concatenate([slots, jnp.broadcast_to(wave, (2, 1))], axis=1)
    short_range = short_range_of(table, before, left, mine, right, after, maps0, maps2)

    spots = positions.astype(jnp.float32)
    half = wavevectors.shape[1] // 2
    waves = lax.dynamic_slice_in_dim(wavevectors, xlo * half, half, axis=1)
    float_waves = waves.astype(jnp.float32)
    own_phases = phases_of(float_waves, spots)
    other_phases = phases_of(float_waves, other_spots)
    partial = jnp.dot(own_phases, latent, preferred_element_type=jnp.float32) + jnp.dot(
        other_phases, other_latent, preferred_element_type=jnp.float32
    )
    owners = ("z", "y")
    count = lax.axis_size(owners)
    lines = 2 * half // count
    pieces = exchanged(partial.astype(jnp.bfloat16).reshape(count, lines, latents), owners)
    factors = jnp.sum(pieces.astype(jnp.float32), axis=0)
    mixed = jnp.dot(factors, mix_weight, precision=lax.Precision.HIGHEST)
    first = lax.rem(lax.axis_index(owners) * lines, half)
    filter_waves = lax.dynamic_slice_in_dim(waves, first, lines, axis=1)
    lengths = jnp.sum(filter_waves * filter_waves, axis=0).astype(jnp.float32)
    gain = jnp.exp(-lengths[:, None] * filter_rate[None, :])
    filtered = (gain * mixed * (1.0 / math.sqrt(NATOMS))).astype(jnp.bfloat16)
    filtered = exchanged(jnp.broadcast_to(filtered, (count, lines, latents)), owners)
    filtered = filtered.reshape(2 * half, latents)

    def back(phases):
        summed = lax.dot_general(
            phases, filtered, (((0,), (0,)), ((), ())), preferred_element_type=jnp.float32
        )
        summed = (summed * (1.0 / math.sqrt(K))).astype(jnp.bfloat16)
        return jnp.dot(summed, out_weight, preferred_element_type=jnp.float32)

    own_message = (back(own_phases) + short_range).astype(jnp.bfloat16)
    other_message = back(other_phases).astype(jnp.bfloat16)
    first_is_mine = xlo == 0
    message = jnp.stack(
        [
            jnp.where(first_is_mine, own_message, other_message),
            jnp.where(first_is_mine, other_message, own_message),
        ]
    )
    message = jnp.moveaxis(message.reshape(2, atoms, wave_devices, part), 2, 1)
    message = exchanged(message.reshape(2 * wave_devices, atoms, part), ("xlo", *WAVES))
    return jnp.sum(message.astype(jnp.float32), axis=0).astype(jnp.bfloat16)


def solution(mesh):
    torus = Mesh(mesh.devices.reshape(8, 2, 8, 2, 2), (*ATOMS, *WAVES))
    placed = (
        P(ATOMS, None),
        P(None, ATOMS),
        P(ATOMS, None),
        P(None, WAVES),
        P(WAVES),
        P(WAVES, None, None),
        P(),
        P(),
        P(),
        P(),
    )

    return jax.shard_map(
        local, mesh=torus, in_specs=placed, out_specs=P(ATOMS, WAVES), check_vma=False
    )
```
